32 devices in a mesh: kpt: 2 (over x), row: 8 (over z, y), col: 2 (over core).
Axes of the slice: x: 2, y: 2, z: 4, core: 2. Of those that a mesh axis runs over, the one named last changes fastest.
Arguments:
- wannier: float32 [64, 32, 1024], P('kpt', ('row', 'col')), parts along dimension 0, may hold values from -6 to 6
- pairs: int32 [384, 2], replicated, may hold values from 0 to 31, as said below
- gmap: int32 [8192], replicated, may hold values from 1 to 32767, as said below
- screened: bfloat16 [4, 2, 8192, 8192], P('kpt', None, 'row', 'col'), parts along dimension 0, may hold values from -0.046875 to 0.046875
Outputs:
- coulomb: float32 [2, 2, 768, 384], P(None, None, ('kpt', 'row', 'col')), parts along dimension 2
The draws below stay inside these ranges and needn't reach their ends.
There are 2 independent parts, one for each index of `kpt`. The reference program is written for one: setup_inputs(seed, part) draws one part's arguments, and reference() takes and returns one part's arrays. A program takes and returns all parts, laid end to end along the dimension named above; an argument that names none is the same for every part. Nothing has to cross between parts.
Inputs may be any that keep to these rules, and one draw needn't show every extreme that they name: `gmap`: 8192 distinct flat cells of the grid; cell 0 is never among them. `pairs`: in each row the first Wannier function is no greater than the second; no two rows are equal.
All inputs are finite; a program needn't handle non-finite values.
Results may differ from the reference program's by a relative error of at most 0.0082.
Values may be sent and summed in bfloat16 or wider, within the bound.
A program may use at most 128 MiB of HBM per device.

```python
import jax
import jax.numpy as jnp
from jax import lax

NW = 32
GX = 32
NG = 8192
NF = 2
NP = 384
GYZ = 1024


def draw_gmap(key, part):
    order = jax.random.permutation(key, GX * GX * GX - 1)
    return (order[:NG] + 1).astype(jnp.int32)


def draw_pairs(key, part):
    upper = jnp.triu_indices(NW)
    first_all = jnp.asarray(upper[0]).astype(jnp.int32)
    second_all = jnp.asarray(upper[1]).astype(jnp.int32)
    order = jax.random.permutation(jax.random.fold_in(key, 17), first_all.shape[0])
    chosen = order[:NP]
    return jnp.stack([first_all[chosen], second_all[chosen]], axis=1).astype(jnp.int32)


def block_scale(stream_key, dims, pieces, low, largest):
    level, own = 1.0, jax.random.fold_in(stream_key, 6)
    for position, blocks in pieces:
        draws = jnp.exp(jax.random.uniform(jax.random.fold_in(own, position), (blocks,), jnp.float32, low / len(pieces), largest / len(pieces)))
        level = level * jnp.repeat(draws, dims[position] // blocks).reshape([-1 if axis == position else 1 for axis in range(len(dims))])
    return level


def gaussian(own_key, shape, width, most, shards=(), dtype=jnp.bfloat16):
    values = width * jax.random.normal(own_key, shape, jnp.float32)
    if shards:
        values = values * block_scale(own_key, shape, shards, -0.22, 0.18)
    return jnp.clip(values, -most, most).astype(dtype)


def setup_inputs(seed: int = 0, part: int = 0) -> dict:
    streams_of = jax.random.split(jax.random.key(seed), 5)
    part_splits = jax.random.split(jax.random.fold_in(streams_of[4], part), 5)
    wannier = gaussian(part_splits[0], (NW, GX, GYZ), 1.0, 6.0, ((1, 16),), jnp.float32)
    pairs = draw_pairs(jax.random.fold_in(streams_of[4], 71), part)
    gmap = draw_gmap(jax.random.fold_in(streams_of[4], 71), part)
    screened = gaussian(part_splits[3], (NF, 2, NG, NG), (2 * NG) ** -0.5, 0.046875, ((2, 8), (3, 2)))
    return dict(wannier=wannier, pairs=pairs, gmap=gmap, screened=screened)


def reference(wannier, pairs, gmap, screened):
    grid = wannier.reshape(NW, GX, GX, GX)
    density = grid[pairs[:, 0]] * grid[pairs[:, 1]]
    spectrum = jnp.fft.fftn(density, axes=(1, 2, 3), norm='ortho').reshape(NP, GX * GX * GX)
    chosen = jnp.take(spectrum, gmap, axis=1)
    rho_real = jnp.real(chosen).astype(jnp.bfloat16)
    rho_imag = jnp.imag(chosen).astype(jnp.bfloat16)
    left_real = rho_real.astype(jnp.float32)
    left_imag = rho_imag.astype(jnp.float32)
    highest = lax.Precision.HIGHEST
    results = []
    for frequency in range(NF):
        w_real = screened[frequency, 0]
        w_imag = screened[frequency, 1]
        mixed_real = jnp.dot(w_real, rho_real.T, preferred_element_type=jnp.float32) - jnp.dot(w_imag, rho_imag.T, preferred_element_type=jnp.float32)
        mixed_imag = jnp.dot(w_real, rho_imag.T, preferred_element_type=jnp.float32) + jnp.dot(w_imag, rho_real.T, preferred_element_type=jnp.float32)
        u_real = jnp.dot(left_real, mixed_real, precision=highest) + jnp.dot(left_imag, mixed_imag, precision=highest)
        u_imag = jnp.dot(left_real, mixed_imag, precision=highest) - jnp.dot(left_imag, mixed_real, precision=highest)
        results.append(jnp.stack([u_real, u_imag], axis=0))
    return jnp.stack(results, axis=0) / jnp.sqrt(jnp.float32(NG))
```

```python
import functools
import math

import jax
import jax.numpy as jnp
from jax import lax
from jax.experimental import pallas as pl
from jax.experimental.pallas import tpu as pltpu
from jax.sharding import PartitionSpec as P

IM = 64
LANES = 128


def twiddle(re, im, c, s):
    if s == 0.0:
        return re, im
    if im is None:
        return re * c, re * (-s)
    if c == 0.0:
        return im * s, re * (-s)
    return re * c + im * s, im * c - re * s


def real_dft(xs):
    n = len(xs)
    if n == 1:
        return [(xs[0], None)]
    if n == 2:
        return [(xs[0] + xs[1], None), (xs[0] - xs[1], None)]
    even, odd = real_dft(xs[0::2]), real_dft(xs[1::2])
    out = [None] * (n // 2 + 1)
    for k in range(n // 4 + 1):
        er, ei = even[k]
        if 4 * k == n:
            c, s = 0.0, 1.0
        elif k == 0:
            c, s = 1.0, 0.0
        else:
            c, s = math.cos(2 * math.pi * k / n), math.sin(2 * math.pi * k / n)
        if c == 0.0 and odd[k][1] is None:
            tr, ti = None, odd[k][0] * -1.0
        else:
            tr, ti = twiddle(odd[k][0], odd[k][1], c, s)
        hi_r = er if tr is None else er + tr
        lo_r = er if tr is None else er - tr
        if ei is None and ti is None:
            hi_i = lo_i = None
        elif ei is None:
            hi_i, lo_i = ti, ti
        elif ti is None:
            hi_i, lo_i = ei, -ei
        else:
            hi_i, lo_i = ei + ti, ti - ei
        out[k] = (hi_r, hi_i)
        if n // 2 - k != k:
            out[n // 2 - k] = (lo_r, lo_i)
    return out


def rho_kernel(norm, index_ref, sel_ref, grid_ref, table_ref, sign_ref, out_ref, dens, spec, cells, rows):
    planes, _, area = grid_ref.shape
    padded = sel_ref.shape[0] // 2
    half = planes // 2 + 1
    groups = spec.shape[0] // 2

    def plane(x, carry):
        both = jnp.dot(sel_ref[...], grid_ref[x], preferred_element_type=jnp.float32)
        dens[x] = both[:padded] * both[padded:]
        return carry

    lax.fori_loop(0, planes, plane, 0)
    for k in range(spec.shape[0]):
        if k >= half:
            spec[k] = jnp.zeros(spec.shape[1:], spec.dtype)
        else:
            if padded < IM:
                pad = jnp.zeros((IM - padded, 2 * area), spec.dtype)
                spec[k, padded:IM] = pad
                spec[k, IM + padded :] = pad

    def chunk(i, carry):
        p0 = pl.multiple_of((i // (area // LANES)) * 16, 16)
        n0 = pl.multiple_of((i % (area // LANES)) * LANES, LANES)
        n1 = pl.multiple_of(n0 + area, LANES)
        p1 = pl.multiple_of(p0 + IM, 16)
        terms = [dens[x, pl.ds(p0, 16), pl.ds(n0, LANES)] for x in range(planes)]
        for k, (re, im) in enumerate(real_dft(terms)):
            re = re * norm
            im = jnp.zeros_like(re) if im is None else im * norm
            re_b, im_b = re.astype(jnp.bfloat16), im.astype(jnp.bfloat16)
            spec[k, pl.ds(p0, 16), pl.ds(n0, LANES)] = re_b
            spec[k, pl.ds(p0, 16), pl.ds(n1, LANES)] = im_b
            spec[k, pl.ds(p1, 16), pl.ds(n0, LANES)] = im_b
            spec[k, pl.ds(p1, 16), pl.ds(n1, LANES)] = (-re).astype(jnp.bfloat16)
        return carry

    lax.fori_loop(0, (padded // 16) * (area // LANES), chunk, 0)
    tile = 256
    steps = area // tile

    def product(i, carry):
        k = (i // steps) * 2
        m0 = pl.multiple_of((i % steps) * tile, tile)
        right = spec[pl.ds(k, 2)].reshape(2 * LANES, 2 * area)
        got = lax.dot_general(
            table_ref[pl.ds(m0, tile), :], right, (((1,), (1,)), ((), ())), preferred_element_type=jnp.float32
        )
        first = pl.multiple_of(k * area + m0, tile)
        second = pl.multiple_of(first + area, tile)
        cells[pl.ds(first, tile), :] = got[:, :LANES]
        cells[pl.ds(second, tile), :] = got[:, LANES:]
        return carry

    lax.fori_loop(0, groups * steps, product, 0)
    count = rows.shape[0]
    unroll = 16

    def pick(i, carry):
        base = pl.multiple_of(i * unroll, unroll)
        for j in range(unroll):
            rows[pl.ds(base + j, 1), :] = cells[pl.ds(index_ref[base + j], 1), :]
        return carry

    lax.fori_loop(0, count // unroll, pick, 0)
    span = 256

    def turn(i, carry):
        g0 = pl.multiple_of(i * span, span)
        flipped = rows[pl.ds(g0, span), :].T
        out_ref[0, :, pl.ds(g0, span)] = flipped[:padded].astype(jnp.bfloat16)
        signed = flipped[IM : IM + padded] * sign_ref[:, pl.ds(g0, span)]
        out_ref[1, :, pl.ds(g0, span)] = signed.astype(jnp.bfloat16)
        return carry

    lax.fori_loop(0, count // span, turn, 0)


def pair_coefficients(grid, table, sel, index, sign):
    planes, _, area = grid.shape
    padded = sel.shape[0] // 2
    count = index.shape[0]
    half = planes // 2 + 1
    even_half = half + half % 2
    norm = 1.0 / math.sqrt(planes * area)
    whole = pl.BlockSpec(memory_space=pltpu.VMEM)
    return pl.pallas_call(
        functools.partial(rho_kernel, norm),
        out_shape=jax.ShapeDtypeStruct((2, padded, count), jnp.bfloat16),
        in_specs=[pl.BlockSpec(memory_space=pltpu.SMEM), whole, whole, whole, whole],
        out_specs=whole,
        scratch_shapes=[
            pltpu.VMEM((planes, padded, area), jnp.float32),
            pltpu.VMEM((even_half, LANES, 2 * area), jnp.bfloat16),
            pltpu.VMEM((even_half * area, LANES), jnp.float32),
            pltpu.VMEM((count, LANES), jnp.float32),
        ],
        compiler_params=pltpu.CompilerParams(vmem_limit_bytes=60 * 1024 * 1024),
        cost_estimate=pl.CostEstimate(flops=10**10, bytes_accessed=8 * 1024 * 1024, transcendentals=0),
        name="rho",
    )(index, sel, grid, table, sign)


def element_kernel(scale, w_ref, right_ref, left_ref, out_ref, right):
    members, parts, owned, _ = right_ref.shape
    pairs = members * owned

    @pl.when((pl.program_id(0) == 0) & (pl.program_id(1) == 0))
    def _():
        for r in range(members):
            for c in range(parts):
                right[c * pairs + r * owned : c * pairs + (r + 1) * owned, :] = right_ref[r, c]

    nt = (((1,), (1,)), ((), ()))
    z_real = lax.dot_general(w_ref[0, 0], right[...], nt, preferred_element_type=jnp.float32)
    z_imag = lax.dot_general(w_ref[0, 1], right[...], nt, preferred_element_type=jnp.float32)
    s_real = (z_real[:, :pairs] - z_imag[:, pairs:]) * scale
    s_imag = (z_real[:, pairs:] + z_imag[:, :pairs]) * scale
    one = jnp.concatenate([s_real, s_imag], axis=1).astype(jnp.bfloat16)
    two = jnp.concatenate([s_imag, -s_real], axis=1).astype(jnp.bfloat16)
    got = jnp.dot(left_ref[0], one, preferred_element_type=jnp.float32)
    got += jnp.dot(left_ref[1], two, preferred_element_type=jnp.float32)

    @pl.when(pl.program_id(1) == 0)
    def _():
        out_ref[0] = got

    @pl.when(pl.program_id(1) > 0)
    def _():
        out_ref[0] += got


def matrix_elements(screened, right, left, scale):
    freqs, parts, rows, columns = screened.shape
    pairs = left.shape[1]
    tile = min(256, rows)
    return pl.pallas_call(
        functools.partial(element_kernel, scale),
        grid=(freqs, rows // tile),
        out_shape=jax.ShapeDtypeStruct((freqs, pairs, parts * pairs), jnp.float32),
        in_specs=[
            pl.BlockSpec((1, parts, tile, columns), lambda f, i: (f, 0, i, 0)),
            pl.BlockSpec(memory_space=pltpu.VMEM),
            pl.BlockSpec((parts, pairs, tile), lambda f, i: (0, 0, i)),
        ],
        out_specs=pl.BlockSpec((1, pairs, parts * pairs), lambda f, i: (f, 0, 0)),
        scratch_shapes=[pltpu.VMEM((parts * pairs, columns), jnp.bfloat16)],
        compiler_params=pltpu.CompilerParams(
            dimension_semantics=("arbitrary", "arbitrary"), vmem_limit_bytes=60 * 1024 * 1024
        ),
        cost_estimate=pl.CostEstimate(
            flops=8 * freqs * rows * columns * pairs, bytes_accessed=2 * screened.size, transcendentals=0
        ),
        name="elements",
    )(screened, right, left)


def plane_table(area):
    side = math.isqrt(area)
    k = lax.broadcasted_iota(jnp.int32, (area, 2 * area), 0)
    n = lax.broadcasted_iota(jnp.int32, (area, 2 * area), 1)
    cell = n % area
    turn = (k // side) * (cell // side) + (k % side) * (cell % side)
    turn = (turn - jnp.where(n >= area, side // 4, 0)) % side
    return jnp.cos(turn.astype(jnp.float32) * (2.0 * math.pi / side)).astype(jnp.bfloat16)


def shards(wannier, pairs, gmap, screened):
    functions, _, area = wannier.shape
    side = math.isqrt(area)
    count = pairs.shape[0]
    members = lax.axis_size("row")
    columns = screened.shape[3]
    row_span = screened.shape[2]
    row, col = lax.axis_index("row"), lax.axis_index("col")
    owned = count // members
    padded = -(-owned // 16) * 16

    local = jnp.swapaxes(wannier, 0, 1).astype(jnp.bfloat16)
    grid = lax.all_gather(local, ("row", "col"), axis=0, tiled=True)
    depth = grid.shape[0]

    mine = lax.dynamic_slice_in_dim(pairs, row * owned, owned, 0)
    mine = jnp.pad(mine, ((0, padded - owned), (0, 0)), constant_values=-1)
    sel = (mine.T.reshape(-1, 1) == jnp.arange(functions, dtype=jnp.int32)[None, :]).astype(jnp.bfloat16)

    flat = lax.dynamic_slice_in_dim(gmap, col * columns, columns, 0)
    kx, ky, kz = flat // area, (flat // side) % side, flat % side
    far = kx > depth // 2
    kx = jnp.where(far, depth - kx, kx)
    ky = jnp.where(far, (side - ky) % side, ky)
    kz = jnp.where(far, (side - kz) % side, kz)
    index = kx * area + ky * side + kz
    sign = jnp.where(far, -1.0, 1.0).astype(jnp.float32)[None, :]

    rho = pair_coefficients(grid, plane_table(area), sel, index, sign)[:, :owned]
    right = lax.all_gather(rho, "row", axis=0, tiled=False)

    start = row * row_span
    block = lax.dynamic_slice_in_dim(right, start % columns, row_span, 3)
    swap = [(i, (i + 1) % lax.axis_size("col")) for i in range(lax.axis_size("col"))]
    other = lax.ppermute(block, "col", swap)
    left = jnp.where(start // columns == col, block, other)
    left = jnp.swapaxes(left, 0, 1).reshape(2, count, row_span)

    partial = matrix_elements(screened, right, left, 1.0 / math.sqrt(gmap.shape[0]))
    freqs = partial.shape[0]
    devices = lax.axis_size(("row", "col"))
    share = count // devices
    pieces = partial.astype(jnp.bfloat16).reshape(freqs, devices, share, 2 * count)
    pieces = jnp.swapaxes(pieces, 0, 1)
    arrived = lax.all_to_all(pieces, ("row", "col"), split_axis=0, concat_axis=0, tiled=True)
    summed = jnp.sum(arrived.astype(jnp.float32), axis=0)
    return summed.reshape(freqs, share, 2, count).transpose(0, 2, 1, 3)


def solution(mesh):
    return jax.shard_map(
        shards,
        mesh=mesh,
        in_specs=(P("kpt", ("row", "col"), None), P(), P(), P("kpt", None, "row", "col")),
        out_specs=P(None, None, ("kpt", "row", "col"), None),
        check_vma=False,
    )
```

```python
import functools
import math

import jax
import jax.numpy as jnp
from jax import lax
from jax.experimental import pallas as pl
from jax.experimental.pallas import tpu as pltpu
from jax.sharding import PartitionSpec as P


IM = 64
LANES = 128


def twiddle(re, im, c, s):
    if s == 0.0:
        return re, im
    if im is None:
        return re * c, re * (-s)
    if c == 0.0:
        return im * s, re * (-s)
    return re * c + im * s, im * c - re * s


def real_dft(xs):
    n = len(xs)
    if n == 1:
        return [(xs[0], None)]
    if n == 2:
        return [(xs[0] + xs[1], None), (xs[0] - xs[1], None)]
    even, odd = real_dft(xs[0::2]), real_dft(xs[1::2])
    out = [None] * (n // 2 + 1)
    for k in range(n // 4 + 1):
        er, ei = even[k]
        if 4 * k == n:
            c, s = 0.0, 1.0
        elif k == 0:
            c, s = 1.0, 0.0
        else:
            c, s = math.cos(2 * math.pi * k / n), math.sin(2 * math.pi * k / n)
        if c == 0.0 and odd[k][1] is None:
            tr, ti = None, odd[k][0] * -1.0
        else:
            tr, ti = twiddle(odd[k][0], odd[k][1], c, s)
        hi_r = er if tr is None else er + tr
        lo_r = er if tr is None else er - tr
        if ei is None and ti is None:
            hi_i = lo_i = None
        elif ei is None:
            hi_i, lo_i = ti, ti
        elif ti is None:
            hi_i, lo_i = ei, -ei
        else:
            hi_i, lo_i = ei + ti, ti - ei
        out[k] = (hi_r, hi_i)
        if n // 2 - k != k:
            out[n // 2 - k] = (lo_r, lo_i)
    return out


def rho_kernel(norm, index_ref, sel_ref, grid_ref, table_ref, sign_ref, out_ref, dens, spec, cells, rows):
    planes, _, area = grid_ref.shape
    padded = sel_ref.shape[0] // 2
    half = planes // 2 + 1
    groups = spec.shape[0] // 2

    def plane(x, carry):
        both = jnp.dot(sel_ref[...], grid_ref[x], preferred_element_type=jnp.float32)
        dens[x] = both[:padded] * both[padded:]
        return carry

    lax.fori_loop(0, planes, plane, 0)
    for k in range(spec.shape[0]):
        if k >= half:
            spec[k] = jnp.zeros(spec.shape[1:], spec.dtype)
        else:
            if padded < IM:
                pad = jnp.zeros((IM - padded, 2 * area), spec.dtype)
                spec[k, padded:IM] = pad
                spec[k, IM + padded :] = pad

    def chunk(i, carry):
        p0 = pl.multiple_of((i // (area // LANES)) * 16, 16)
        n0 = pl.multiple_of((i % (area // LANES)) * LANES, LANES)
        n1 = pl.multiple_of(n0 + area, LANES)
        p1 = pl.multiple_of(p0 + IM, 16)
        terms = [dens[x, pl.ds(p0, 16), pl.ds(n0, LANES)] for x in range(planes)]
        for k, (re, im) in enumerate(real_dft(terms)):
            re = re * norm
            im = jnp.zeros_like(re) if im is None else im * norm
            re_b, im_b = re.astype(jnp.bfloat16), im.astype(jnp.bfloat16)
            spec[k, pl.ds(p0, 16), pl.ds(n0, LANES)] = re_b
            spec[k, pl.ds(p0, 16), pl.ds(n1, LANES)] = im_b
            spec[k, pl.ds(p1, 16), pl.ds(n0, LANES)] = im_b
            spec[k, pl.ds(p1, 16), pl.ds(n1, LANES)] = (-re).astype(jnp.bfloat16)
        return carry

    lax.fori_loop(0, (padded // 16) * (area // LANES), chunk, 0)
    tile = 256
    steps = area // tile

    def product(i, carry):
        k = (i // steps) * 2
        m0 = pl.multiple_of((i % steps) * tile, tile)
        right = spec[pl.ds(k, 2)].reshape(2 * LANES, 2 * area)
        got = lax.dot_general(
            table_ref[pl.ds(m0, tile), :], right, (((1,), (1,)), ((), ())), preferred_element_type=jnp.float32
        )
        first = pl.multiple_of(k * area + m0, tile)
        second = pl.multiple_of(first + area, tile)
        cells[pl.ds(first, tile), :] = got[:, :LANES]
        cells[pl.ds(second, tile), :] = got[:, LANES:]
        return carry

    lax.fori_loop(0, groups * steps, product, 0)
    count = rows.shape[0]
    unroll = 16

    def pick(i, carry):
        base = pl.multiple_of(i * unroll, unroll)
        for j in range(unroll):
            rows[pl.ds(base + j, 1), :] = cells[pl.ds(index_ref[base + j], 1), :]
        return carry

    lax.fori_loop(0, count // unroll, pick, 0)
    span = 256

    def turn(i, carry):
        g0 = pl.multiple_of(i * span, span)
        flipped = rows[pl.ds(g0, span), :].T
        out_ref[0, :, pl.ds(g0, span)] = flipped[:padded].astype(jnp.bfloat16)
        signed = flipped[IM : IM + padded] * sign_ref[:, pl.ds(g0, span)]
        out_ref[1, :, pl.ds(g0, span)] = signed.astype(jnp.bfloat16)
        return carry

    lax.fori_loop(0, count // span, turn, 0)


def pair_coefficients(grid, table, sel, index, sign):
    planes, _, area = grid.shape
    padded = sel.shape[0] // 2
    count = index.shape[0]
    half = planes // 2 + 1
    even_half = half + half % 2
    norm = 1.0 / math.sqrt(planes * area)
    whole = pl.BlockSpec(memory_space=pltpu.VMEM)
    return pl.pallas_call(
        functools.partial(rho_kernel, norm),
        out_shape=jax.ShapeDtypeStruct((2, padded, count), jnp.bfloat16),
        in_specs=[pl.BlockSpec(memory_space=pltpu.SMEM), whole, whole, whole, whole],
        out_specs=whole,
        scratch_shapes=[
            pltpu.VMEM((planes, padded, area), jnp.float32),
            pltpu.VMEM((even_half, LANES, 2 * area), jnp.bfloat16),
            pltpu.VMEM((even_half * area, LANES), jnp.float32),
            pltpu.VMEM((count, LANES), jnp.float32),
        ],
        compiler_params=pltpu.CompilerParams(vmem_limit_bytes=60 * 1024 * 1024),
        cost_estimate=pl.CostEstimate(flops=10**10, bytes_accessed=8 * 1024 * 1024, transcendentals=0),
        name="rho",
    )(index, sel, grid, table, sign)


def stack_pairs(right_ref, right):
    members, parts, owned, _ = right_ref.shape
    pairs = members * owned
    for r in range(members):
        for c in range(parts):
            right[c * pairs + r * owned : c * pairs + (r + 1) * owned, :] = right_ref[r, c]


def screened_terms(w_ref, right, pairs):
    nt = (((1,), (1,)), ((), ()))
    z_real = lax.dot_general(w_ref[0, 0], right[...], nt, preferred_element_type=jnp.float32)
    z_imag = lax.dot_general(w_ref[0, 1], right[...], nt, preferred_element_type=jnp.float32)
    return z_real[:, :pairs] - z_imag[:, pairs:], z_real[:, pairs:] + z_imag[:, :pairs]


def first_kernel(w_ref, right_ref, out_ref, right):
    pairs = right_ref.shape[0] * right_ref.shape[2]

    @pl.when((pl.program_id(0) == 0) & (pl.program_id(1) == 0))
    def _():
        stack_pairs(right_ref, right)

    s_real, s_imag = screened_terms(w_ref, right, pairs)
    out_ref[0, :, :pairs] = s_real
    out_ref[0, :, pairs:] = s_imag


def element_kernel(scale, w_ref, right_ref, left_ref, first_ref, out_ref, right):
    pairs = right_ref.shape[0] * right_ref.shape[2]

    @pl.when((pl.program_id(0) == 0) & (pl.program_id(1) == 0))
    def _():
        stack_pairs(right_ref, right)

    s_real, s_imag = screened_terms(w_ref, right, pairs)
    s_real = (s_real + first_ref[0, :, :pairs]) * scale
    s_imag = (s_imag + first_ref[0, :, pairs:]) * scale
    one = jnp.concatenate([s_real, s_imag], axis=1).astype(jnp.bfloat16)
    two = jnp.concatenate([s_imag, -s_real], axis=1).astype(jnp.bfloat16)
    got = jnp.dot(left_ref[0], one, preferred_element_type=jnp.float32)
    got += jnp.dot(left_ref[1], two, preferred_element_type=jnp.float32)

    @pl.when(pl.program_id(1) == 0)
    def _():
        out_ref[0] = got

    @pl.when(pl.program_id(1) > 0)
    def _():
        out_ref[0] += got


def kernel_options(screened, right):
    freqs, parts, rows, _ = screened.shape
    width = right.shape[3]
    pairs = right.shape[0] * right.shape[2]
    return dict(
        scratch_shapes=[pltpu.VMEM((parts * pairs, width), jnp.bfloat16)],
        compiler_params=pltpu.CompilerParams(
            dimension_semantics=("arbitrary", "arbitrary"), vmem_limit_bytes=60 * 1024 * 1024
        ),
        cost_estimate=pl.CostEstimate(
            flops=8 * freqs * rows * width * pairs,
            bytes_accessed=2 * freqs * parts * rows * width,
            transcendentals=0,
        ),
    )


def first_columns(screened, right):
    freqs, parts, rows, _ = screened.shape
    pairs, width = right.shape[0] * right.shape[2], right.shape[3]
    tile = min(256, rows)
    return pl.pallas_call(
        first_kernel,
        grid=(freqs, rows // tile),
        out_shape=jax.ShapeDtypeStruct((freqs, rows, parts * pairs), jnp.float32),
        in_specs=[
            pl.BlockSpec((1, parts, tile, width), lambda f, i: (f, 0, i, 0)),
            pl.BlockSpec(memory_space=pltpu.VMEM),
        ],
        out_specs=pl.BlockSpec((1, tile, parts * pairs), lambda f, i: (f, i, 0)),
        name="first_columns",
        **kernel_options(screened, right),
    )(screened, right)


def matrix_elements(screened, right, left, first, scale):
    freqs, parts, rows, columns = screened.shape
    pairs, width = left.shape[1], right.shape[3]
    tile = min(256, rows)
    last = columns // width - 1
    return pl.pallas_call(
        functools.partial(element_kernel, scale),
        grid=(freqs, rows // tile),
        out_shape=jax.ShapeDtypeStruct((freqs, pairs, parts * pairs), jnp.float32),
        in_specs=[
            pl.BlockSpec((1, parts, tile, width), lambda f, i: (f, 0, i, last)),
            pl.BlockSpec(memory_space=pltpu.VMEM),
            pl.BlockSpec((parts, pairs, tile), lambda f, i: (0, 0, i)),
            pl.BlockSpec((1, tile, parts * pairs), lambda f, i: (f, i, 0)),
        ],
        out_specs=pl.BlockSpec((1, pairs, parts * pairs), lambda f, i: (f, 0, 0)),
        name="elements",
        **kernel_options(screened, right),
    )(screened, right, left, first)


def plane_table(area):
    side = math.isqrt(area)
    k = lax.broadcasted_iota(jnp.int32, (area, 2 * area), 0)
    n = lax.broadcasted_iota(jnp.int32, (area, 2 * area), 1)
    cell = n % area
    turn = (k // side) * (cell // side) + (k % side) * (cell % side)
    turn = (turn - jnp.where(n >= area, side // 4, 0)) % side
    return jnp.cos(turn.astype(jnp.float32) * (2.0 * math.pi / side)).astype(jnp.bfloat16)


def shards(wannier, pairs, gmap, screened):
    functions, _, area = wannier.shape
    side = math.isqrt(area)
    count = pairs.shape[0]
    members = lax.axis_size("row")
    columns = screened.shape[3]
    row_span = screened.shape[2]
    row, col = lax.axis_index("row"), lax.axis_index("col")
    owned = count // members
    padded = -(-owned // 16) * 16

    local = jnp.swapaxes(wannier, 0, 1).astype(jnp.bfloat16)
    grid = lax.all_gather(local, ("row", "col"), axis=0, tiled=True)
    depth = grid.shape[0]

    mine = lax.dynamic_slice_in_dim(pairs, row * owned, owned, 0)
    mine = jnp.pad(mine, ((0, padded - owned), (0, 0)), constant_values=-1)
    sel = (mine.T.reshape(-1, 1) == jnp.arange(functions, dtype=jnp.int32)[None, :]).astype(jnp.bfloat16)

    flat = lax.dynamic_slice_in_dim(gmap, col * columns, columns, 0)
    kx, ky, kz = flat // area, (flat // side) % side, flat % side
    far = kx > depth // 2
    kx = jnp.where(far, depth - kx, kx)
    ky = jnp.where(far, (side - ky) % side, ky)
    kz = jnp.where(far, (side - kz) % side, kz)
    index = kx * area + ky * side + kz
    sign = jnp.where(far, -1.0, 1.0).astype(jnp.float32)[None, :]

    rho = pair_coefficients(grid, plane_table(area), sel, index, sign)[:, :owned]
    cut = columns - columns // 4
    early = lax.all_gather(rho[:, :, :cut], "row", axis=0, tiled=False)
    late = lax.all_gather(rho[:, :, cut:], "row", axis=0, tiled=False)
    first = first_columns(screened, early)

    start = row * row_span
    at = start % columns
    block = jnp.where(
        at < cut,
        lax.dynamic_slice_in_dim(early, jnp.minimum(at, cut - row_span), row_span, 3),
        lax.dynamic_slice_in_dim(late, jnp.maximum(at - cut, 0), row_span, 3),
    )
    swap = [(i, (i + 1) % lax.axis_size("col")) for i in range(lax.axis_size("col"))]
    other = lax.ppermute(block, "col", swap)
    left = jnp.where(start // columns == col, block, other)
    left = jnp.swapaxes(left, 0, 1).reshape(2, count, row_span)

    partial = matrix_elements(screened, late, left, first, 1.0 / math.sqrt(gmap.shape[0]))
    freqs = partial.shape[0]
    devices = lax.axis_size(("row", "col"))
    share = count // devices
    pieces = partial.astype(jnp.bfloat16).reshape(freqs, devices, share, 2 * count)
    pieces = jnp.swapaxes(pieces, 0, 1)
    arrived = lax.all_to_all(pieces, ("row", "col"), split_axis=0, concat_axis=0, tiled=True)
    summed = jnp.sum(arrived.astype(jnp.float32), axis=0)
    return summed.reshape(freqs, share, 2, count).transpose(0, 2, 1, 3)


def solution(mesh):
    return jax.shard_map(
        shards,
        mesh=mesh,
        in_specs=(P("kpt", ("row", "col"), None), P(), P(), P("kpt", None, "row", "col")),
        out_specs=P(None, None, ("kpt", "row", "col"), None),
        check_vma=False,
    )
```
